32 devices in a mesh: rep: 4 (over x, y), dp: 8 (over z, core).
Axes of the slice: x: 2, y: 2, z: 4, core: 2. Of those that a mesh axis runs over, the one named last changes fastest.
Arguments:
- x: bfloat16 [32, 2048, 640], P(('rep', 'dp')), parts along dimension 0
- dy: bfloat16 [32, 2048, 640], P(('rep', 'dp')), parts along dimension 0
- w_gate: bfloat16 [2, 640, 2048], replicated
- w_up: bfloat16 [2, 640, 2048], replicated
- w_down: bfloat16 [2, 2048, 640], replicated
- m_w_gate: float32 [2, 640, 2048], P(None, 'dp')
- m_w_up: float32 [2, 640, 2048], P(None, 'dp')
- m_w_down: float32 [2, 2048, 640], P(None, 'dp')
- v_w_gate: float32 [2, 640, 2048], P(None, 'dp')
- v_w_up: float32 [2, 640, 2048], P(None, 'dp')
- v_w_down: float32 [2, 2048, 640], P(None, 'dp')
Outputs:
- output 1: bfloat16 [8, 640, 2048], P('rep'), parts along dimension 0
- output 2: bfloat16 [8, 640, 2048], P('rep'), parts along dimension 0
- output 3: bfloat16 [8, 2048, 640], P('rep'), parts along dimension 0
- output 4: float32 [8, 640, 2048], P('rep', 'dp'), parts along dimension 0
- output 5: float32 [8, 640, 2048], P('rep', 'dp'), parts along dimension 0
- output 6: float32 [8, 2048, 640], P('rep', 'dp'), parts along dimension 0
- output 7: float32 [8, 640, 2048], P('rep', 'dp'), parts along dimension 0
- output 8: float32 [8, 640, 2048], P('rep', 'dp'), parts along dimension 0
- output 9: float32 [8, 2048, 640], P('rep', 'dp'), parts along dimension 0
There are 4 independent parts. The reference program is written for one: setup_inputs(seed, part) draws one part's arguments, and reference() takes and returns one part's arrays. A program takes and returns all parts, laid end to end along the dimension named above; an argument that names none is the same for every part.
All inputs are finite; a program needn't handle non-finite values.
Results may differ from the reference program's by a relative error of at most 0.022.
Values are sent between devices in bfloat16 or wider.
A program may use at most 2 GiB of HBM per device.

```python
import jax
import jax.numpy as jnp
from jax import lax

SEQUENCES = 8
TOKENS = 2048
D = 640
FF = 2048
LAYERS = 2
NAMES = ("w_gate", "w_up", "w_down")
SHAPES = {"w_gate": (LAYERS, D, FF), "w_up": (LAYERS, D, FF), "w_down": (LAYERS, FF, D)}


def bump(key, n, height):
    away = (jnp.arange(n, dtype=jnp.int32) - jax.random.randint(key, (), 0, n, jnp.int32)) % n
    return jnp.where(away < n // 8, height, 1.0)


def together(key, own, strength):
    shared = jax.random.normal(key, own.shape[1:], jnp.float32)
    return (own + strength * shared) * lax.rsqrt(1 + strength * strength)


def setup_inputs(seed: int = 0, part: int = 0) -> dict:
    kx, kdy, ka, kb, kz, kf, kh, kl, *keys = jax.random.split(jax.random.key(seed), 8 + 3 * len(NAMES))
    kx, kdy, ka, kb = (jax.random.fold_in(k, part) for k in (kx, kdy, ka, kb))
    kw, km, kv = (keys[i::3] for i in range(3))
    shape = (SEQUENCES, TOKENS, D)
    much_x, much_dy = jax.random.uniform(kz, (2,), jnp.float32, 0.0, 1.0)
    loud = 2.0 ** jax.random.uniform(jax.random.fold_in(kz, 1), (), jnp.float32, -1.0, 2.0)
    layers = 2.0 ** jax.random.uniform(kl, (LAYERS, 1, 1), jnp.float32, -1.0, 1.0)
    x = together(ka, jax.random.normal(kx, shape, jnp.float32), much_x) * bump(kf, D, 4.0)
    dy = together(kb, jax.random.normal(kdy, shape, jnp.float32), much_dy)
    drawn = {"x": x.astype(jnp.bfloat16), "dy": (loud * dy * (SEQUENCES * TOKENS) ** -0.5).astype(jnp.bfloat16)}
    for key, name in zip(kw, NAMES, strict=True):
        w = jax.random.normal(key, SHAPES[name], jnp.float32) * SHAPES[name][1] ** -0.5
        drawn[name] = (w * {"w_gate": 1.0, "w_up": bump(kh, FF, 4.0), "w_down": layers}[name]).astype(jnp.bfloat16)
    for key, name in zip(km, NAMES, strict=True):
        drawn[f"m_{name}"] = 0.1 * jax.random.normal(key, SHAPES[name], jnp.float32)
    for key, name in zip(kv, NAMES, strict=True):
        drawn[f"v_{name}"] = jax.random.uniform(key, SHAPES[name], jnp.float32, 0.005, 0.015)
    return drawn


def matmul(a, w):
    return jnp.dot(a, w, preferred_element_type=jnp.float32).astype(jnp.bfloat16)


def normed(h):
    wide = h.astype(jnp.float32)
    scale = lax.rsqrt(jnp.mean(wide**2, -1, keepdims=True) + 1e-6)
    return (wide * scale).astype(jnp.bfloat16)


def layer(h, w):
    a = normed(h)
    gate = jnp.dot(a, w["w_gate"], preferred_element_type=jnp.float32)
    up = jnp.dot(a, w["w_up"], preferred_element_type=jnp.float32)
    return h + matmul((jax.nn.silu(gate) * up).astype(jnp.bfloat16), w["w_down"])


def adamw(w, m, v, g):
    m = 0.9 * m + 0.1 * g
    v = 0.95 * v + 0.05 * g * g
    step = m * lax.rsqrt(v + 1e-8) + 0.1 * w
    return (w - 0.02 * step).astype(jnp.bfloat16), m, v


def clipped(gradients, sum_of_squares, count):
    factor = jnp.minimum(1.0, 0.5 * lax.rsqrt(sum_of_squares / count + 1e-30))
    return [g * factor for g in gradients]


def stack(weights, h):
    return lax.scan(lambda h, w: (layer(h, w), None), h, weights)[0]


def reference(x, dy, w_gate, w_up, w_down, m_w_gate, m_w_up, m_w_down, v_w_gate, v_w_up, v_w_down):
    weights = dict(zip(NAMES, (w_gate, w_up, w_down), strict=True))

    def take(so_far, sequence):
        h, by_y = sequence
        _, back = jax.vjp(lambda w: stack(w, h), weights)
        return jax.tree.map(lambda total, term: total + term.astype(jnp.float32), so_far, back(by_y)[0]), None

    none_yet = {name: jnp.zeros(w.shape, jnp.float32) for name, w in weights.items()}
    by_weights, _ = lax.scan(take, none_yet, (x, dy))
    gradients = [by_weights[name].astype(jnp.bfloat16).astype(jnp.float32) for name in NAMES]
    gradients = clipped(gradients, sum(jnp.sum(g * g) for g in gradients), sum(g.size for g in gradients))
    new = [
        adamw(w.astype(jnp.float32), m, v, g)
        for w, m, v, g in zip((w_gate, w_up, w_down), (m_w_gate, m_w_up, m_w_down), (v_w_gate, v_w_up, v_w_down), gradients, strict=True)
    ]
    return tuple(one[which] for which in range(3) for one in new)
```

```python
import functools

import jax
import jax.numpy as jnp
from jax import lax
from jax.experimental import pallas as pl
from jax.experimental.pallas import tpu as pltpu
from jax.sharding import PartitionSpec as P

NAMES = ("w_gate", "w_up", "w_down")
MESH = pl.DeviceIdType.MESH
F32, BF16 = jnp.float32, jnp.bfloat16
ORDER = ((1, 2), (1, 0), (1, 1), (0, 2), (0, 0), (0, 1))
N = len(ORDER)


def chunks(rows, body):
    @pl.loop(0, rows // 16)
    def _(t):
        body(pl.ds(pl.multiple_of(t * 16, 16), 16))


def comm_kernel(count, *refs):
    grads, refs = refs[:N], refs[N:]
    w_in, m_in, v_in, refs = refs[:3], refs[3:6], refs[6:9], refs[9:]
    full, m_out, v_out, refs = refs[:3], refs[3:6], refs[6:9], refs[9:]
    xs, rs, olds, refs = refs[:3], refs[3:6], refs[6:9], refs[9:]
    squares, norms, fill_sem, load_sem, x_send, x_recv, r_send, r_recv, n_send, n_recv, g_send, g_recv = refs

    rep, me = lax.axis_index("rep"), lax.axis_index("dp")
    z, k = me // 2, lax.rem(me, 2)
    flip = z >= 2
    inner = jnp.logical_or(z == 1, z == 2)
    outer = jnp.logical_not(inner)

    def blk(mirrored):
        return jnp.where(flip, 3 - mirrored, mirrored)

    own = jnp.where(inner, blk(1), blk(0))
    ahead = jnp.where(flip, z - 1, z + 1)
    back = jnp.where(outer, z, jnp.where(flip, z + 1, z - 1))

    def device(zz, kk):
        return (rep, 2 * zz + kk)

    def remote(src, dst, send, recv, to):
        return pltpu.make_async_remote_copy(
            src_ref=src, dst_ref=dst, send_sem=send, recv_sem=recv, device_id=to, device_id_type=MESH
        )

    def load(i):
        layer, which = ORDER[i]
        rows = m_in[which].shape[1]
        return (
            pltpu.make_async_copy(m_in[which].at[layer], m_out[which].at[layer], load_sem.at[i, 0]),
            pltpu.make_async_copy(v_in[which].at[layer], v_out[which].at[layer], load_sem.at[i, 1]),
            pltpu.make_async_copy(
                w_in[which].at[layer, pl.ds(pl.multiple_of(me * rows, 16), rows)], olds[which].at[layer], load_sem.at[i, 2]
            ),
        )

    def fill(i):
        layer, which = ORDER[i]
        return pltpu.make_async_copy(grads[i], full[which].at[layer], fill_sem.at[i])

    def exchange(i):
        layer, which = ORDER[i]
        return remote(full[which].at[layer, :, 1 - k], xs[which].at[layer], x_send.at[i], x_recv.at[i], device(z, 1 - k))

    def hop(i, block, slot, send, to):
        layer, which = ORDER[i]
        return remote(
            full[which].at[layer, block, k], rs[which].at[layer, slot], r_send.at[i, send], r_recv.at[i, slot], device(to, k)
        )

    def add(i, block, slots):
        layer, which = ORDER[i]
        mine, x, r = full[which].at[layer, block, k], xs[which].at[layer, block], rs[which].at[layer]

        def body(at):
            total = mine[at, :].astype(F32) + x[at, :].astype(F32)
            for slot in slots:
                total += r[slot, at, :].astype(F32)
            mine[at, :] = total.astype(BF16)

        chunks(mine.shape[0], body)

    def finish(i):
        layer, which = ORDER[i]
        mine = full[which].at[layer, own, k]

        @pl.when(outer)
        def _():
            hop(i, blk(0), 0, 0, ahead).wait_recv()
            add(i, own, (0,))

        @pl.when(inner)
        def _():
            hop(i, blk(1), 2, 2, ahead).wait_recv()
            hop(i, blk(1), 4, 2, ahead).wait_recv()
            add(i, own, (2, 4))

        def body(at):
            g = mine[at, :].astype(F32)
            g = g * g
            total = squares[...]
            for c in range(g.shape[1] // 128):
                total += g[:8, c * 128 : (c + 1) * 128] + g[8:, c * 128 : (c + 1) * 128]
            squares[...] = total

        chunks(mine.shape[0], body)

    for i in range(N):
        fill(i).start()
    squares[...] = jnp.zeros_like(squares)

    barrier = pltpu.get_barrier_semaphore()
    for p in range(1, 8):
        pl.semaphore_signal(barrier, inc=1, device_id=(rep, lax.rem(me + p, 8)), device_id_type=MESH)
    pl.semaphore_wait(barrier, 7)

    for i in range(N):
        fill(i).wait()
        exchange(i).start()
    for i in range(N):
        for copy in load(i):
            copy.start()

    for i in range(N):
        exchange(i).wait_recv()

        @pl.when(outer)
        def _():
            for j in range(3):
                add(i, blk(3 - j), ())
                hop(i, blk(3 - j), j, j, ahead).start()

        @pl.when(inner)
        def _():
            hop(i, blk(3), 0, 0, ahead).wait_recv()
            add(i, blk(3), (0,))
            hop(i, blk(3), 3, 0, ahead).start()
            hop(i, blk(2), 1, 1, ahead).wait_recv()
            add(i, blk(2), (1,))
            hop(i, blk(2), 4, 1, ahead).start()
            hop(i, blk(0), 3, 2, ahead).wait_recv()
            add(i, blk(0), (3,))
            hop(i, blk(0), 0, 2, back).start()

        if i >= 1:
            finish(i - 1)
    finish(N - 1)
    for i in range(N):
        exchange(i).wait_send()
        for j in range(3):
            hop(i, blk(0), 0, j, ahead).wait_send()

    norms[me] = squares[...]

    def norm(p, src):
        return remote(norms.at[src], norms.at[src], n_send.at[p - 1], n_recv.at[src], (rep, lax.rem(me + p, 8)))

    for p in range(1, 8):
        norm(p, me).start()
    for p in range(1, 8):
        norm(p, lax.rem(me + p, 8)).wait_recv()
    total = norms[0]
    for d in range(1, 8):
        total += norms[d]
    ss = jnp.sum(total, keepdims=True)
    factor = jnp.minimum(1.0, 0.5 * lax.rsqrt(ss / count + 1e-30))

    def update(i):
        layer, which = ORDER[i]
        for copy in load(i):
            copy.wait()
        mine, m, v, w = full[which].at[layer, own, k], m_out[which].at[layer], v_out[which].at[layer], olds[which].at[layer]

        def body(at):
            g = mine[at, :].astype(F32) * factor
            new_m = 0.9 * m[at, :] + 0.1 * g
            new_v = 0.95 * v[at, :] + 0.05 * g * g
            old = w[at, :].astype(F32)
            step = new_m * lax.rsqrt(new_v + 1e-8) + 0.1 * old
            m[at, :] = new_m
            v[at, :] = new_v
            mine[at, :] = (old - 0.02 * step).astype(BF16)

        chunks(mine.shape[0], body)

    def pass_on(i, block, which_way, to, plane):
        layer, which = ORDER[i]
        here = full[which].at[layer, block, plane]
        return remote(here, here, g_send.at[i, block, which_way], g_recv.at[i, block, plane], to)

    def ahead_copy(i, block):
        return pass_on(i, block, 0, device(ahead, k), k)

    def back_copy(i, block):
        return pass_on(i, block, 1, device(back, k), k)

    def across_copy(i, block):
        return pass_on(i, block, 2, device(z, 1 - k), k)

    for s in range(N + 3):
        if s < N:
            update(s)

            @pl.when(inner)
            def _():
                back_copy(s, own).start()

            ahead_copy(s, own).start()
            across_copy(s, own).start()
        if 0 <= s - 1 < N:
            i = s - 1

            @pl.when(outer)
            def _():
                ahead_copy(i, blk(1)).wait_recv()
                across_copy(i, blk(1)).start()

            @pl.when(inner)
            def _():
                ahead_copy(i, blk(2)).wait_recv()
                back_copy(i, blk(2)).start()
                across_copy(i, blk(2)).start()
                ahead_copy(i, blk(0)).wait_recv()
                ahead_copy(i, blk(0)).start()
                across_copy(i, blk(0)).start()

        if 0 <= s - 2 < N:
            i = s - 2

            @pl.when(outer)
            def _():
                ahead_copy(i, blk(2)).wait_recv()
                across_copy(i, blk(2)).start()

            @pl.when(inner)
            def _():
                ahead_copy(i, blk(3)).wait_recv()
                back_copy(i, blk(3)).start()
                across_copy(i, blk(3)).start()

        if 0 <= s - 3 < N:
            i = s - 3

            @pl.when(outer)
            def _():
                ahead_copy(i, blk(3)).wait_recv()
                across_copy(i, blk(3)).start()

    for p in range(1, 8):
        norm(p, me).wait_send()
    for i in range(N):
        for b in range(4):
            pass_on(i, b, 2, device(z, 1 - k), 1 - k).wait_recv()
            across_copy(i, b).wait_send()
        ahead_copy(i, own).wait_send()

        @pl.when(inner)
        def _():
            ahead_copy(i, blk(0)).wait_send()
            for b in range(1, 4):
                back_copy(i, blk(b)).wait_send()


def shapes_of(w):
    layers, rows, columns = w.shape
    return layers, rows // 8, columns


def exchange_and_update(grads, weights, ms, vs):
    dims = [shapes_of(w) for w in weights]
    count = float(sum(w.size for w in weights))
    any_space = pl.BlockSpec(memory_space=pl.ANY)
    vmem = pl.BlockSpec(memory_space=pltpu.VMEM)
    grads = [grads[layer][which] for layer, which in ORDER]
    grads = [g.reshape(4, 2, g.shape[0] // 8, g.shape[1]) for g in grads]
    dma = pltpu.SemaphoreType.DMA
    out = pl.pallas_call(
        functools.partial(comm_kernel, count),
        out_shape=[jax.ShapeDtypeStruct((l, 4, 2, r, c), BF16) for l, r, c in dims]
        + [jax.ShapeDtypeStruct(d, F32) for d in dims] * 2,
        in_specs=[any_space] * (N + 9),
        out_specs=[vmem] * 9,
        scratch_shapes=[pltpu.VMEM((l, 4, r, c), BF16) for l, r, c in dims]
        + [pltpu.VMEM((l, 5, r, c), BF16) for l, r, c in dims]
        + [pltpu.VMEM(d, BF16) for d in dims]
        + [
            pltpu.VMEM((8, 128), F32),
            pltpu.VMEM((8, 8, 128), F32),
            dma((N,)),
            dma((N, 3)),
            dma((N,)),
            dma((N,)),
            dma((N, 3)),
            dma((N, 5)),
            dma((7,)),
            dma((8,)),
            dma((N, 4, 3)),
            dma((N, 4, 2)),
        ],
        compiler_params=pltpu.CompilerParams(collective_id=0, has_side_effects=True, vmem_limit_bytes=60 * 2**20),
        name="reduce_step_gather",
    )(*grads, *weights, *ms, *vs)
    new_w = [o.reshape(w.shape) for o, w in zip(out[:3], weights)]
    return (*new_w, *out[3:])


def matmul(a, w):
    return jnp.dot(a, w, preferred_element_type=jnp.float32).astype(jnp.bfloat16)


def normed(h):
    wide = h.astype(jnp.float32)
    scale = lax.rsqrt(jnp.mean(wide**2, -1, keepdims=True) + 1e-6)
    return (wide * scale).astype(jnp.bfloat16)


def layer(h, w):
    a = normed(h)
    gate = jnp.dot(a, w[0], preferred_element_type=jnp.float32)
    up = jnp.dot(a, w[1], preferred_element_type=jnp.float32)
    return h + matmul((jax.nn.silu(gate) * up).astype(jnp.bfloat16), w[2])


def stack(weights, h):
    for w in weights:
        h = layer(h, w)
    return h


def gradients(x, dy, weights):
    each = [[w[number] for w in weights] for number in range(2)]
    return jax.vjp(lambda w: stack(w, x), each)[1](dy)[0]


def solution(mesh):
    def step(x, dy, *arrays):
        weights, ms, vs = (arrays[i : i + 3] for i in (0, 3, 6))
        return exchange_and_update(gradients(x[0], dy[0], weights), weights, ms, vs)

    every, rows, whole = P(("rep", "dp")), P(None, "dp"), P(None)
    return jax.shard_map(
        step,
        mesh=mesh,
        in_specs=(every, every, whole, whole, whole) + (rows,) * 6,
        out_specs=(P("rep"),) * 3 + (P("rep", "dp"),) * 6,
        check_vma=False,
    )
```

```python
import functools

import jax
import jax.numpy as jnp
from jax import lax
from jax.experimental import pallas as pl
from jax.experimental.pallas import tpu as pltpu
from jax.sharding import PartitionSpec as P

NAMES = ("w_gate", "w_up", "w_down")
MESH = pl.DeviceIdType.MESH
F32, BF16 = jnp.float32, jnp.bfloat16
ORDER = ((1, 2), (1, 0), (1, 1), (0, 2), (0, 0), (0, 1))
N = len(ORDER)


def chunks(rows, body):
    @pl.loop(0, rows // 16)
    def _(t):
        body(pl.ds(pl.multiple_of(t * 16, 16), 16))


TOKENS, D, FF = 2048, 640, 2048
T, CH = 256, 512
PARTS = FF // CH
STATIC_UNROLL = 2


def nt(a, b):
    return lax.dot_general(a, b, (((1,), (1,)), ((), ())), preferred_element_type=F32)


def nn(a, b):
    return jnp.dot(a, b, preferred_element_type=F32)


def tile(t, size=T):
    return pl.ds(pl.multiple_of(t * size, size), size)


def scale_of(wide):
    return lax.rsqrt(jnp.mean(wide * wide, -1, keepdims=True) + 1e-6)


def compute(x_hbm, dy_hbm, w_hbm, full, h, a, a_t, d, d_t, acc, hid, dgate, dup, wg, wu, wd, in_sem, w_sem, after_tile, after_part):
    def weights(number):
        layer = jnp.where(number // PARTS == 1, 1, 0)
        at, slot = tile(lax.rem(number, PARTS), CH), lax.rem(number, 2)
        return (
            pltpu.make_async_copy(w_hbm[0].at[layer, :, at], wg.at[slot], w_sem.at[slot, 0]),
            pltpu.make_async_copy(w_hbm[1].at[layer, :, at], wu.at[slot], w_sem.at[slot, 1]),
            pltpu.make_async_copy(w_hbm[2].at[layer, at, :], wd.at[slot], w_sem.at[slot, 2]),
        )

    def next_weights(number):
        for copy in weights(number):
            copy.wait()

        @pl.when(number + 1 < 3 * PARTS)
        def _():
            for copy in weights(number + 1):
                copy.start()

        return lax.rem(number, 2)

    def norm_tile(at, wide):
        value = (wide * scale_of(wide)).astype(BF16)
        a[at, :] = value
        a_t[:, at] = value.T

    load_x = pltpu.make_async_copy(x_hbm, h, in_sem.at[0])
    load_dy = pltpu.make_async_copy(dy_hbm, d, in_sem.at[1])
    load_x.start()
    load_dy.start()
    for copy in weights(0):
        copy.start()
    load_x.wait()

    @pl.loop(0, TOKENS // T)
    def _(t):
        wide = h[tile(t), :].astype(F32)
        a[tile(t), :] = (wide * scale_of(wide)).astype(BF16)

    @pl.loop(0, PARTS)
    def _(c):
        slot = next_weights(c)

        def forward(t, first):
            at = tile(t)
            gate, up = nn(a[at, :], wg[slot]), nn(a[at, :], wu[slot])
            value = nn((gate * jax.nn.sigmoid(gate) * up).astype(BF16), wd[slot])
            if first:
                acc[at, :] = value
            else:
                acc[at, :] += value

        @pl.when(c == 0)
        def _():
            @pl.loop(0, TOKENS // T, unroll=STATIC_UNROLL)
            def _(t):
                forward(t, True)

        @pl.when(c > 0)
        def _():
            @pl.loop(0, TOKENS // T, unroll=STATIC_UNROLL)
            def _(t):
                forward(t, False)

    load_dy.wait()

    @pl.loop(0, TOKENS // T)
    def _(t):
        at = tile(t)
        value = h[at, :].astype(F32) + acc[at, :].astype(BF16).astype(F32)
        value = value.astype(BF16)
        h[at, :] = value
        norm_tile(at, value.astype(F32))
        d_t[:, at] = d[at, :].T
        acc[at, :] = jnp.zeros((T, D), F32)

    def backward(layer):
        @pl.loop(0, PARTS)
        def _(c):
            number = (2 - layer) * PARTS + c
            slot = next_weights(number)

            @pl.loop(0, TOKENS // T // STATIC_UNROLL)
            def _(pair):
                for half in range(STATIC_UNROLL):
                    at = tile(pair * STATIC_UNROLL + half)
                    gate, up = nn(a[at, :], wg[slot]), nn(a[at, :], wu[slot])
                    back = nt(d[at, :], wd[slot]).astype(BF16).astype(F32)
                    sig = jax.nn.sigmoid(gate)
                    silu = gate * sig
                    hid[at, :] = (silu * up).astype(BF16)
                    by_up = (back * silu).astype(BF16)
                    by_gate = (back * up * (sig + silu * (1.0 - sig))).astype(BF16)
                    dup[at, :] = by_up
                    dgate[at, :] = by_gate
                    if layer == 1:
                        acc[at, :] += nt(by_gate, wg[slot]) + nt(by_up, wu[slot])
                after_tile(number - PARTS, pair)

            @pl.loop(0, CH // 256)
            def _(n):
                here = tile(n, 256)
                there = pl.ds(pl.multiple_of(c * CH + n * 256, 256), 256)
                full[2][layer, c, n] = nn(d_t[...], hid[:, here]).astype(BF16).T
                full[0][layer, :, :, :, there] = nn(a_t[...], dgate[:, here]).astype(BF16).reshape(4, 2, D // 8, 256)
                full[1][layer, :, :, :, there] = nn(a_t[...], dup[:, here]).astype(BF16).reshape(4, 2, D // 8, 256)

            after_part(number - PARTS)

    backward(1)

    @pl.loop(0, TOKENS // T)
    def _(t):
        at = tile(t)
        wide = h[at, :].astype(F32)
        scale = scale_of(wide)
        by_a = acc[at, :].astype(BF16).astype(F32)
        by_h = scale * by_a - wide * (scale * scale * scale * jnp.mean(by_a * wide, -1, keepdims=True))
        value = (d[at, :].astype(F32) + by_h.astype(BF16).astype(F32)).astype(BF16)
        d[at, :] = value
        d_t[:, at] = value.T

    load_x.start()
    load_x.wait()

    @pl.loop(0, TOKENS // T)
    def _(t):
        norm_tile(tile(t), h[tile(t), :].astype(F32))

    backward(0)


COMPUTE_SCRATCH = [
    pltpu.VMEM((TOKENS, D), BF16),
    pltpu.VMEM((TOKENS, D), BF16),
    pltpu.VMEM((D, TOKENS), BF16),
    pltpu.VMEM((TOKENS, D), BF16),
    pltpu.VMEM((D, TOKENS), BF16),
    pltpu.VMEM((TOKENS, D), F32),
    pltpu.VMEM((TOKENS, CH), BF16),
    pltpu.VMEM((TOKENS, CH), BF16),
    pltpu.VMEM((TOKENS, CH), BF16),
    pltpu.VMEM((2, D, CH), BF16),
    pltpu.VMEM((2, D, CH), BF16),
    pltpu.VMEM((2, CH, D), BF16),
    pltpu.SemaphoreType.DMA((2,)),
    pltpu.SemaphoreType.DMA((2, 3)),
]


LAG = 2
UNITS = 2 * PARTS


def step_kernel(count, x_hbm, dy_hbm, *refs):
    w_in, m_in, v_in, refs = refs[:3], refs[3:6], refs[6:9], refs[9:]
    full, m_out, v_out, refs = refs[:3], refs[3:6], refs[6:9], refs[9:]
    scratch, refs = refs[: len(COMPUTE_SCRATCH)], refs[len(COMPUTE_SCRATCH) :]
    xs, rs, refs = refs[:3], refs[3:6], refs[6:]
    moments, squares, norms, load_sem, store_sem, x_send, x_recv, r_send, r_recv, n_send, n_recv, g_send, g_recv = refs
    a, a_t, acc = scratch[1], scratch[2], scratch[5]

    rep, me = lax.axis_index("rep"), lax.axis_index("dp")
    z, k = me // 2, lax.rem(me, 2)
    flip = z >= 2
    inner = jnp.logical_or(z == 1, z == 2)
    outer = jnp.logical_not(inner)

    def blk(mirrored):
        return jnp.where(flip, 3 - mirrored, mirrored)

    own = jnp.where(inner, blk(1), blk(0))
    ahead = jnp.where(flip, z - 1, z + 1)
    back = jnp.where(outer, z, jnp.where(flip, z + 1, z - 1))

    def device(zz, kk):
        return (rep, 2 * zz + kk)

    def remote(src, dst, send, recv, to):
        return pltpu.make_async_remote_copy(
            src_ref=src, dst_ref=dst, send_sem=send, recv_sem=recv, device_id=to, device_id_type=MESH
        )


    def place(u):
        c = lax.rem(u, PARTS)
        return 1 - u // PARTS, c, tile(c, CH)

    def exchange(u):
        layer, c, at = place(u)
        to = device(z, 1 - k)
        return [
            remote(full[m].at[layer, :, 1 - k, :, at], xs[m].at[layer, :, :, at], x_send.at[u, m], x_recv.at[u, m], to)
            for m in range(2)
        ] + [remote(full[2].at[layer, c, 1 - k], xs[2].at[layer, c], x_send.at[u, 2], x_recv.at[u, 2], to)]

    def hop(u, m, block, slot, send, to):
        layer, c, at = place(u)
        sems = r_send.at[u, m, send], r_recv.at[u, m, slot], device(to, k)
        if m == 2:
            return remote(full[2].at[layer, c, k], rs[2].at[layer, slot], *sems)
        return remote(full[m].at[layer, block, k, :, at], rs[m].at[layer, slot, :, at], *sems)

    def each(u, block, body):
        body(0)
        body(1)

        @pl.when(lax.rem(u, PARTS) == block)
        def _():
            body(2)

    def add(u, m, block, slots, square=False):
        layer, c, at = place(u)

        def part(rows, columns):
            x = xs[m][layer, block, rows, columns]
            total = full[m][layer, block, k, rows, columns].astype(F32) + x.astype(F32)
            for slot in slots:
                total += rs[m][layer, slot, rows, columns].astype(F32)
            total = total.astype(BF16)
            full[m][layer, block, k, rows, columns] = total
            if square:
                total = total.astype(F32)
                total = total * total
                folded = total[:8]
                for r in range(1, total.shape[0] // 8):
                    folded += total[r * 8 : (r + 1) * 8]
                sums = squares[...]
                for q in range(total.shape[1] // 128):
                    sums += folded[:, q * 128 : (q + 1) * 128]
                squares[...] = sums

        if m < 2:
            part(pl.ds(0, D // 8), at)
        else:

            @pl.loop(0, 4)
            def _(q):
                part(tile(q, FF // 32), pl.ds(0, D))

    def send_out(u):
        for copy in exchange(u):
            copy.wait_recv()

        @pl.when(outer)
        def _():
            for j in range(3):

                def body(m):
                    add(u, m, blk(3 - j), ())
                    hop(u, m, blk(3 - j), j, j, ahead).start()

                each(u, blk(3 - j), body)

    def pass_sum(u, j):
        block, come, go, to = ((3, 0, 3, ahead), (2, 1, 4, ahead), (0, 3, 0, back))[j]

        @pl.when(inner)
        def _():
            def body(m):
                hop(u, m, blk(block), come, j, ahead).wait_recv()
                add(u, m, blk(block), (come,))
                hop(u, m, blk(block), go, j, to).start()

            each(u, blk(block), body)

    def finish(u):
        @pl.when(outer)
        def _():
            def body(m):
                hop(u, m, own, 0, 0, ahead).wait_recv()
                add(u, m, own, (0,), True)

            each(u, own, body)

        @pl.when(inner)
        def _():
            def body(m):
                hop(u, m, own, 2, 2, ahead).wait_recv()
                hop(u, m, own, 4, 2, ahead).wait_recv()
                add(u, m, own, (2, 4), True)

            each(u, own, body)

    def sent(u):
        for copy in exchange(u):
            copy.wait_send()

        @pl.when(outer)
        def _():
            for j in range(3):
                each(u, blk(3 - j), lambda m: hop(u, m, blk(3 - j), j, j, ahead).wait_send())

        @pl.when(inner)
        def _():
            for j, block in enumerate((3, 2, 0)):
                each(u, blk(block), lambda m: hop(u, m, blk(block), 0, j, ahead).wait_send())

    def after_part(u):
        for copy in exchange(u):
            copy.start()

    def beside(u, p):
        @pl.when(jnp.logical_and(p == 0, u >= 1))
        def _():
            send_out(u - 1)

        @pl.when(jnp.logical_and(p == 1, u >= LAG))
        def _():
            pass_sum(u - LAG, 0)

        @pl.when(jnp.logical_and(p == 2, u >= LAG))
        def _():
            pass_sum(u - LAG, 1)

        @pl.when(jnp.logical_and(p == 2, u >= LAG + 1))
        def _():
            finish(u - LAG - 1)

        @pl.when(jnp.logical_and(p == 3, u >= LAG))
        def _():
            pass_sum(u - LAG, 2)

    squares[...] = jnp.zeros_like(squares)
    barrier = pltpu.get_barrier_semaphore()
    for p in range(1, 8):
        pl.semaphore_signal(barrier, inc=1, device_id=(rep, lax.rem(me + p, 8)), device_id_type=MESH)
    pl.semaphore_wait(barrier, 7)

    compute(x_hbm, dy_hbm, w_in, full, *scratch, beside, after_part)


    def holds(i):
        layer, which = ORDER[i]
        if which == 2:
            first = 512 * layer
            return acc.at[first : first + 256], acc.at[first + 256 : first + 512], a.at[256 * layer : 256 * layer + 256]
        old = (2 * layer + which) * (D // 8)
        return moments.at[which, 0], moments.at[which, 1], a_t.at[old : old + D // 8]

    def load(i):
        layer, which = ORDER[i]
        rows = m_in[which].shape[1]
        m, v, old = holds(i)
        return (
            pltpu.make_async_copy(m_in[which].at[layer], m, load_sem.at[i, 0]),
            pltpu.make_async_copy(v_in[which].at[layer], v, load_sem.at[i, 1]),
            pltpu.make_async_copy(w_in[which].at[layer, pl.ds(pl.multiple_of(me * rows, 16), rows)], old, load_sem.at[i, 2]),
        )

    def store(i):
        layer, which = ORDER[i]
        m, v, _ = holds(i)
        return (
            pltpu.make_async_copy(m, m_out[which].at[layer], store_sem.at[i, 0]),
            pltpu.make_async_copy(v, v_out[which].at[layer], store_sem.at[i, 1]),
        )

    for i in range(4):
        for copy in load(i):
            copy.start()

    send_out(UNITS - 1)
    for u in range(UNITS - LAG, UNITS):
        for j in range(3):
            pass_sum(u, j)
        finish(u - 1)
    finish(UNITS - 1)

    @pl.loop(0, UNITS)
    def _(u):
        sent(u)

    norms[me] = squares[...]

    def norm(p, src):
        return remote(norms.at[src], norms.at[src], n_send.at[p - 1], n_recv.at[src], (rep, lax.rem(me + p, 8)))

    for p in range(1, 8):
        norm(p, me).start()
    for p in range(1, 8):
        norm(p, lax.rem(me + p, 8)).wait_recv()
    total = norms[0]
    for other in range(1, 8):
        total += norms[other]
    ss = jnp.sum(total, keepdims=True)
    factor = jnp.minimum(1.0, 0.5 * lax.rsqrt(ss / count + 1e-30))

    def update(i):
        layer, which = ORDER[i]
        for copy in load(i):
            copy.wait()
        mine = full[which].at[layer, own, k]
        m, v, w = holds(i)

        def body(at):
            g = mine[at, :].astype(F32) * factor
            new_m = 0.9 * m[at, :] + 0.1 * g
            new_v = 0.95 * v[at, :] + 0.05 * g * g
            old = w[at, :].astype(F32)
            step = new_m * lax.rsqrt(new_v + 1e-8) + 0.1 * old
            m[at, :] = new_m
            v[at, :] = new_v
            mine[at, :] = (old - 0.02 * step).astype(BF16)

        chunks(mine.shape[0], body)
        for copy in store(i):
            copy.start()

    def pass_on(i, block, which_way, to, plane):
        layer, which = ORDER[i]
        here = full[which].at[layer, block, plane]
        return remote(here, here, g_send.at[i, block, which_way], g_recv.at[i, block, plane], to)

    def ahead_copy(i, block):
        return pass_on(i, block, 0, device(ahead, k), k)

    def back_copy(i, block):
        return pass_on(i, block, 1, device(back, k), k)

    def across_copy(i, block):
        return pass_on(i, block, 2, device(z, 1 - k), k)

    for s in range(N + 3):
        if s < N:
            if s >= 4:
                for copy in store(s - 3):
                    copy.wait()
                for copy in load(s):
                    copy.start()
            update(s)

            @pl.when(inner)
            def _():
                back_copy(s, own).start()

            ahead_copy(s, own).start()
            across_copy(s, own).start()
        if 0 <= s - 1 < N:
            i = s - 1

            @pl.when(outer)
            def _():
                ahead_copy(i, blk(1)).wait_recv()
                across_copy(i, blk(1)).start()

            @pl.when(inner)
            def _():
                ahead_copy(i, blk(2)).wait_recv()
                back_copy(i, blk(2)).start()
                across_copy(i, blk(2)).start()
                ahead_copy(i, blk(0)).wait_recv()
                ahead_copy(i, blk(0)).start()
                across_copy(i, blk(0)).start()

        if 0 <= s - 2 < N:
            i = s - 2

            @pl.when(outer)
            def _():
                ahead_copy(i, blk(2)).wait_recv()
                across_copy(i, blk(2)).start()

            @pl.when(inner)
            def _():
                ahead_copy(i, blk(3)).wait_recv()
                back_copy(i, blk(3)).start()
                across_copy(i, blk(3)).start()

        if 0 <= s - 3 < N:
            i = s - 3

            @pl.when(outer)
            def _():
                ahead_copy(i, blk(3)).wait_recv()
                across_copy(i, blk(3)).start()

    for p in range(1, 8):
        norm(p, me).wait_send()
    for i in range(N):
        if i in (0, 3, 4, 5):
            for copy in store(i):
                copy.wait()
        for b in range(4):
            pass_on(i, b, 2, device(z, 1 - k), 1 - k).wait_recv()
            across_copy(i, b).wait_send()
        ahead_copy(i, own).wait_send()

        @pl.when(inner)
        def _():
            ahead_copy(i, blk(0)).wait_send()
            for b in range(1, 4):
                back_copy(i, blk(b)).wait_send()


def solution(mesh):
    def step(x, dy, *arrays):
        weights = arrays[:3]
        dims = [(w.shape[0], w.shape[1] // 8, w.shape[2]) for w in weights]
        count = float(sum(w.size for w in weights))
        any_space = pl.BlockSpec(memory_space=pl.ANY)
        vmem = pl.BlockSpec(memory_space=pltpu.VMEM)
        dma = pltpu.SemaphoreType.DMA
        out = pl.pallas_call(
            functools.partial(step_kernel, count),
            out_shape=[jax.ShapeDtypeStruct((l, 4, 2, r, c), BF16) for l, r, c in dims]
            + [jax.ShapeDtypeStruct(d, F32) for d in dims] * 2,
            in_specs=[any_space] * 11,
            out_specs=[vmem] * 3 + [any_space] * 6,
            scratch_shapes=COMPUTE_SCRATCH
            + [pltpu.VMEM((l, 4, r, c), BF16) for l, r, c in dims]
            + [pltpu.VMEM((l, 5, r, c), BF16) for l, r, c in dims]
            + [
                pltpu.VMEM((2, 2, D // 8, FF), F32),
                pltpu.VMEM((8, 128), F32),
                pltpu.VMEM((8, 8, 128), F32),
                dma((N, 3)),
                dma((N, 2)),
                dma((UNITS, 3)),
                dma((UNITS, 3)),
                dma((UNITS, 3, 3)),
                dma((UNITS, 3, 5)),
                dma((7,)),
                dma((8,)),
                dma((N, 4, 3)),
                dma((N, 4, 2)),
            ],
            compiler_params=pltpu.CompilerParams(collective_id=0, has_side_effects=True, vmem_limit_bytes=67043328),
            name="training_step",
        )(x[0], dy[0], *arrays)
        return tuple(o.reshape(w.shape) for o, w in zip(out[:3], weights)) + tuple(out[3:])

    every, rows, whole = P(("rep", "dp")), P(None, "dp"), P(None)
    return jax.shard_map(
        step,
        mesh=mesh,
        in_specs=(every, every, whole, whole, whole) + (rows,) * 6,
        out_specs=(P("rep"),) * 3 + (P("rep", "dp"),) * 6,
        check_vma=False,
    )
```

```python
import functools

import jax
import jax.numpy as jnp
from jax import lax
from jax.experimental import pallas as pl
from jax.experimental.pallas import tpu as pltpu
from jax.sharding import PartitionSpec as P

NAMES = ("w_gate", "w_up", "w_down")
MESH = pl.DeviceIdType.MESH
F32, BF16 = jnp.float32, jnp.bfloat16
ORDER = ((1, 2), (1, 0), (1, 1), (0, 2), (0, 0), (0, 1))
N = len(ORDER)


def chunks(rows, body):
    @pl.loop(0, rows // 16)
    def _(t):
        body(pl.ds(pl.multiple_of(t * 16, 16), 16))


TOKENS, D, FF = 2048, 640, 2048
T, CH = 512, 512
PARTS = FF // CH
STATIC_UNROLL = 1


def nt(a, b):
    return lax.dot_general(a, b, (((1,), (1,)), ((), ())), preferred_element_type=F32)


def nn(a, b):
    return jnp.dot(a, b, preferred_element_type=F32)


def tile(t, size=T):
    return pl.ds(pl.multiple_of(t * size, size), size)


def scale_of(wide):
    return lax.rsqrt(jnp.mean(wide * wide, -1, keepdims=True) + 1e-6)


def compute(x_hbm, dy_hbm, w_hbm, full, h, a, a_t, d, d_t, acc, hid, dgate, dup, wg, wu, wd, in_sem, w_sem, after_tile, after_part):
    def weights(number):
        layer = jnp.where(number // PARTS == 1, 1, 0)
        at, slot = tile(lax.rem(number, PARTS), CH), lax.rem(number, 2)
        return (
            pltpu.make_async_copy(w_hbm[0].at[layer, :, at], wg.at[slot], w_sem.at[slot, 0]),
            pltpu.make_async_copy(w_hbm[1].at[layer, :, at], wu.at[slot], w_sem.at[slot, 1]),
            pltpu.make_async_copy(w_hbm[2].at[layer, at, :], wd.at[slot], w_sem.at[slot, 2]),
        )

    def next_weights(number):
        for copy in weights(number):
            copy.wait()

        @pl.when(number + 1 < 3 * PARTS)
        def _():
            for copy in weights(number + 1):
                copy.start()

        return lax.rem(number, 2)

    def norm_tile(at, wide):
        value = (wide * scale_of(wide)).astype(BF16)
        a[at, :] = value
        a_t[:, at] = value.T

    load_x = pltpu.make_async_copy(x_hbm, h, in_sem.at[0])
    load_dy = pltpu.make_async_copy(dy_hbm, d, in_sem.at[1])
    load_x.start()
    load_dy.start()
    for copy in weights(0):
        copy.start()
    load_x.wait()

    @pl.loop(0, TOKENS // T)
    def _(t):
        wide = h[tile(t), :].astype(F32)
        a[tile(t), :] = (wide * scale_of(wide)).astype(BF16)

    @pl.loop(0, PARTS)
    def _(c):
        slot = next_weights(c)

        def forward(t, first):
            at = tile(t)
            gate, up = nn(a[at, :], wg[slot]), nn(a[at, :], wu[slot])
            value = nn((gate * jax.nn.sigmoid(gate) * up).astype(BF16), wd[slot])
            if first:
                acc[at, :] = value
            else:
                acc[at, :] += value

        @pl.when(c == 0)
        def _():
            @pl.loop(0, TOKENS // T, unroll=STATIC_UNROLL)
            def _(t):
                forward(t, True)

        @pl.when(c > 0)
        def _():
            @pl.loop(0, TOKENS // T, unroll=STATIC_UNROLL)
            def _(t):
                forward(t, False)

    load_dy.wait()

    @pl.loop(0, TOKENS // T)
    def _(t):
        at = tile(t)
        value = h[at, :].astype(F32) + acc[at, :].astype(BF16).astype(F32)
        value = value.astype(BF16)
        h[at, :] = value
        norm_tile(at, value.astype(F32))
        d_t[:, at] = d[at, :].T
        acc[at, :] = jnp.zeros((T, D), F32)

    def backward(layer):
        @pl.loop(0, PARTS)
        def _(c):
            number = (2 - layer) * PARTS + c
            slot = next_weights(number)

            @pl.loop(0, TOKENS // T // STATIC_UNROLL)
            def _(pair):
                for half in range(STATIC_UNROLL):
                    at = tile(pair * STATIC_UNROLL + half)
                    gate, up = nn(a[at, :], wg[slot]), nn(a[at, :], wu[slot])
                    back = nt(d[at, :], wd[slot]).astype(BF16).astype(F32)
                    sig = jax.nn.sigmoid(gate)
                    silu = gate * sig
                    hid[at, :] = (silu * up).astype(BF16)
                    by_up = (back * silu).astype(BF16)
                    by_gate = (back * up * (sig + silu * (1.0 - sig))).astype(BF16)
                    dup[at, :] = by_up
                    dgate[at, :] = by_gate
                    if layer == 1:
                        acc[at, :] += nt(by_gate, wg[slot]) + nt(by_up, wu[slot])
                after_tile(number - PARTS, pair)

            @pl.loop(0, CH // 256)
            def _(n):
                here = tile(n, 256)
                there = pl.ds(pl.multiple_of(c * CH + n * 256, 256), 256)
                full[2][layer, c, n] = nn(d_t[...], hid[:, here]).astype(BF16).T
                full[0][layer, :, :, :, there] = nn(a_t[...], dgate[:, here]).astype(BF16).reshape(4, 2, D // 8, 256)
                full[1][layer, :, :, :, there] = nn(a_t[...], dup[:, here]).astype(BF16).reshape(4, 2, D // 8, 256)

            after_part(number - PARTS)

    backward(1)

    @pl.loop(0, TOKENS // T)
    def _(t):
        at = tile(t)
        wide = h[at, :].astype(F32)
        scale = scale_of(wide)
        by_a = acc[at, :].astype(BF16).astype(F32)
        by_h = scale * by_a - wide * (scale * scale * scale * jnp.mean(by_a * wide, -1, keepdims=True))
        value = (d[at, :].astype(F32) + by_h.astype(BF16).astype(F32)).astype(BF16)
        d[at, :] = value
        d_t[:, at] = value.T

    load_x.start()
    load_x.wait()

    @pl.loop(0, TOKENS // T)
    def _(t):
        norm_tile(tile(t), h[tile(t), :].astype(F32))

    backward(0)


COMPUTE_SCRATCH = [
    pltpu.VMEM((TOKENS, D), BF16),
    pltpu.VMEM((TOKENS, D), BF16),
    pltpu.VMEM((D, TOKENS), BF16),
    pltpu.VMEM((TOKENS, D), BF16),
    pltpu.VMEM((D, TOKENS), BF16),
    pltpu.VMEM((TOKENS, D), F32),
    pltpu.VMEM((TOKENS, CH), BF16),
    pltpu.VMEM((TOKENS, CH), BF16),
    pltpu.VMEM((TOKENS, CH), BF16),
    pltpu.VMEM((2, D, CH), BF16),
    pltpu.VMEM((2, D, CH), BF16),
    pltpu.VMEM((2, CH, D), BF16),
    pltpu.SemaphoreType.DMA((2,)),
    pltpu.SemaphoreType.DMA((2, 3)),
]


LAG = 2
UNITS = 2 * PARTS
QUARTERS, ROWS = 4, FF // 32
PIECES = 2 + QUARTERS


def step_kernel(count, x_hbm, dy_hbm, *refs):
    w_in, m_in, v_in, refs = refs[:3], refs[3:6], refs[6:9], refs[9:]
    w_out, m_out, v_out, m_lent, v_lent, refs = refs[:3], refs[3:6], refs[6:9], refs[9:12], refs[12:15], refs[15:]
    full, refs = refs[:3], refs[3:]
    scratch, refs = refs[: len(COMPUTE_SCRATCH)], refs[len(COMPUTE_SCRATCH) :]
    xs, rs, refs = refs[:3], refs[3:6], refs[6:]
    moments, squares, norms, load_sem, store_sem, x_send, x_recv, r_send, r_recv, n_send, n_recv, g_send, g_recv, refs = *refs[:13], refs[13:]
    lend_send, lend_recv, sum_send, sum_recv, keep_sem, extra_sem, give_send, give_recv = refs
    a, a_t, acc = scratch[1], scratch[2], scratch[5]

    rep, me = lax.axis_index("rep"), lax.axis_index("dp")
    z, k = me // 2, lax.rem(me, 2)
    flip = z >= 2
    inner = jnp.logical_or(z == 1, z == 2)
    outer = jnp.logical_not(inner)

    def blk(mirrored):
        return jnp.where(flip, 3 - mirrored, mirrored)

    own = jnp.where(inner, blk(1), blk(0))
    ahead = jnp.where(flip, z - 1, z + 1)
    back = jnp.where(outer, z, jnp.where(flip, z + 1, z - 1))

    def device(zz, kk):
        return (rep, 2 * zz + kk)

    def remote(src, dst, send, recv, to):
        return pltpu.make_async_remote_copy(
            src_ref=src, dst_ref=dst, send_sem=send, recv_sem=recv, device_id=to, device_id_type=MESH
        )


    def place(u):
        c = lax.rem(u, PARTS)
        return 1 - u // PARTS, c, tile(c, CH)

    def exchange(u):
        layer, c, at = place(u)
        to = device(z, 1 - k)
        return [
            remote(full[m].at[layer, :, 1 - k, :, at], xs[m].at[layer, :, :, at], x_send.at[u, m], x_recv.at[u, m], to)
            for m in range(2)
        ] + [remote(full[2].at[layer, c, 1 - k], xs[2].at[layer, c], x_send.at[u, 2], x_recv.at[u, 2], to)]

    def hop(u, m, block, slot, send, to):
        layer, c, at = place(u)
        sems = r_send.at[u, m, send], r_recv.at[u, m, slot], device(to, k)
        if m >= 2:
            rows = pl.ds((m - 2) * ROWS, ROWS)
            return remote(full[2].at[layer, c, k, rows], rs[2].at[layer, slot, rows], *sems)
        return remote(full[m].at[layer, block, k, :, at], rs[m].at[layer, slot, :, at], *sems)

    def each(u, block, body):
        body(0)
        body(1)

        @pl.when(lax.rem(u, PARTS) == block)
        def _():
            for m in range(2, PIECES):
                body(m)

    def add(u, m, block, slots, square=False):
        layer, c, at = place(u)
        w = min(m, 2)

        def part(rows, columns):
            x = xs[w][layer, block, rows, columns]
            total = full[w][layer, block, k, rows, columns].astype(F32) + x.astype(F32)
            for slot in slots:
                total += rs[w][layer, slot, rows, columns].astype(F32)
            total = total.astype(BF16)
            full[w][layer, block, k, rows, columns] = total
            if square:
                total = total.astype(F32)
                total = total * total
                folded = total[:8]
                for r in range(1, total.shape[0] // 8):
                    folded += total[r * 8 : (r + 1) * 8]
                sums = squares[...]
                for q in range(total.shape[1] // 128):
                    sums += folded[:, q * 128 : (q + 1) * 128]
                squares[...] = sums

        if m < 2:
            part(pl.ds(0, D // 8), at)
        else:
            part(pl.ds((m - 2) * ROWS, ROWS), pl.ds(0, D))


    def when(condition, body):
        if not isinstance(condition, bool):
            pl.when(condition)(body)
        elif condition:
            body()

    def lend(which):
        to = device(back, k)
        return (
            remote(m_in[which].at[0], m_lent[which], lend_send.at[which, 0], lend_recv.at[which, 0], to),
            remote(v_in[which].at[0], v_lent[which], lend_send.at[which, 1], lend_recv.at[which, 1], to),
        )

    def partial(u, m):
        _, c, at = place(u)
        sems = sum_send.at[c, m], sum_recv.at[c, m], device(back, k)
        if m >= 2:
            rows = pl.ds((m - 2) * ROWS, ROWS)
            return remote(full[2].at[0, c, k, rows], rs[2].at[0, 1, rows], *sems)
        return remote(full[m].at[0, own, k, :, at], rs[m].at[0, 1, :, at], *sems)

    def give(which):
        here = full[which].at[0, blk(1), k]
        return remote(here, rs[which].at[0, 2], give_send.at[which], give_recv.at[which], device(ahead, k))

    def send_out(u):
        for copy in exchange(u):
            copy.wait_recv()

        @pl.when(outer)
        def _():
            for j in range(3):

                def body(m):
                    add(u, m, blk(3 - j), ())
                    hop(u, m, blk(3 - j), j, j, ahead).start()

                when(j < 2 or u < PARTS, lambda: each(u, blk(3 - j), body))

    def pass_sum(u, j):
        block, come, go, to = ((3, 0, 3, ahead), (2, 1, 4, ahead), (0, 3, 0, back))[j]

        @pl.when(inner)
        def _():
            def body(m):
                hop(u, m, blk(block), come, j, ahead).wait_recv()
                add(u, m, blk(block), (come,))
                hop(u, m, blk(block), go, j, to).start()

            each(u, blk(block), body)

    def finish(u):
        @pl.when(outer)
        def _():
            def body(m):
                hop(u, m, own, 0, 0, ahead).wait_recv()
                add(u, m, own, (0,), True)

            each(u, own, body)

            def theirs(m):
                partial(u, m).wait_recv()
                add(u, m, blk(1), (1,), True)

            when(u >= PARTS, lambda: each(u, blk(1), theirs))

        def body(m):
            hop(u, m, own, 2, 2, ahead).wait_recv()
            hop(u, m, own, 4, 2, ahead).wait_recv()
            add(u, m, own, (2, 4), True)

        when(u < PARTS, lambda: pl.when(inner)(lambda: each(u, own, body)))

    def pass_out(u):
        @pl.when(inner)
        def _():
            def body(m):
                hop(u, m, own, 4, 2, ahead).wait_recv()
                add(u, m, own, (4,))
                partial(u, m).start()

            each(u, own, body)

    def sent(u):
        for copy in exchange(u):
            copy.wait_send()

        @pl.when(outer)
        def _():
            for j in range(3):
                when(
                    j < 2 or u < PARTS,
                    lambda: each(u, blk(3 - j), lambda m: hop(u, m, blk(3 - j), j, j, ahead).wait_send()),
                )

        @pl.when(inner)
        def _():
            for j, block in enumerate((3, 2, 0)):
                each(u, blk(block), lambda m: hop(u, m, blk(block), 0, j, ahead).wait_send())
            when(u >= PARTS, lambda: each(u, own, lambda m: partial(u, m).wait_send()))

    def after_part(u):
        for copy in exchange(u):
            copy.start()

    def beside(u, p):
        @pl.when(jnp.logical_and(p == 0, u >= 1))
        def _():
            send_out(u - 1)

        @pl.when(jnp.logical_and(p == 1, u >= LAG))
        def _():
            pass_sum(u - LAG, 0)

        @pl.when(jnp.logical_and(p == 2, u >= LAG))
        def _():
            pass_sum(u - LAG, 1)

        @pl.when(jnp.logical_and(p == 2, u >= LAG + 2))
        def _():
            finish(u - LAG - 2)

        @pl.when(jnp.logical_and(p == 3, u >= LAG + 1))
        def _():
            pass_sum(u - LAG - 1, 2)

        @pl.when(jnp.logical_and(p == 3, u >= LAG + PARTS + 1))
        def _():
            pass_out(u - LAG - 1)

    squares[...] = jnp.zeros_like(squares)
    barrier = pltpu.get_barrier_semaphore()
    for p in range(1, 8):
        pl.semaphore_signal(barrier, inc=1, device_id=(rep, lax.rem(me + p, 8)), device_id_type=MESH)
    pl.semaphore_wait(barrier, 7)

    @pl.when(inner)
    def _():
        for which in range(3):
            for copy in lend(which):
                copy.start()

    compute(x_hbm, dy_hbm, w_in, full, *scratch, beside, after_part)


    def holds(i):
        layer, which = ORDER[i]
        if which == 2:
            first = 512 * layer
            return acc.at[first : first + 256], acc.at[first + 256 : first + 512], a.at[256 * layer : 256 * layer + 256]
        old = (2 * layer + which) * (D // 8)
        return moments.at[0], moments.at[1], a_t.at[old : old + D // 8]

    def load(i):
        layer, which = ORDER[i]
        rows = m_in[which].shape[1]
        m, v, old = holds(i)
        return (
            pltpu.make_async_copy(m_in[which].at[layer], m, load_sem.at[i, 0]),
            pltpu.make_async_copy(v_in[which].at[layer], v, load_sem.at[i, 1]),
            pltpu.make_async_copy(w_in[which].at[layer, pl.ds(pl.multiple_of(me * rows, 16), rows)], old, load_sem.at[i, 2]),
        )

    def store(i):
        layer, which = ORDER[i]
        m, v, _ = holds(i)
        return (
            pltpu.make_async_copy(m, m_out[which].at[layer], store_sem.at[i, 0]),
            pltpu.make_async_copy(v, v_out[which].at[layer], store_sem.at[i, 1]),
        )

    for i in (0, 1, 3):
        for copy in load(i):
            copy.start()

    send_out(UNITS - 1)
    pass_sum(6, 0)
    pass_sum(5, 2)
    pass_out(5)
    pass_sum(6, 1)
    pass_sum(7, 0)
    pass_sum(6, 2)
    pass_out(6)
    finish(4)
    pass_sum(7, 1)
    finish(5)
    pass_sum(7, 2)
    pass_out(7)
    finish(6)
    finish(7)

    @pl.loop(0, UNITS)
    def _(u):
        sent(u)

    norms[me] = squares[...]

    def norm(p, src):
        return remote(norms.at[src], norms.at[src], n_send.at[p - 1], n_recv.at[src], (rep, lax.rem(me + p, 8)))

    for p in range(1, 8):
        norm(p, me).start()
    for p in range(1, 8):
        norm(p, lax.rem(me + p, 8)).wait_recv()
    total = norms[0]
    for other in range(1, 8):
        total += norms[other]
    ss = jnp.sum(total, keepdims=True)
    factor = jnp.minimum(1.0, 0.5 * lax.rsqrt(ss / count + 1e-30))

    def step_block(grad, m, v, w, new):
        def body(at):
            g = grad[at, :].astype(F32) * factor
            new_m = 0.9 * m[at, :] + 0.1 * g
            new_v = 0.95 * v[at, :] + 0.05 * g * g
            old = w[at, :].astype(F32)
            step = new_m * lax.rsqrt(new_v + 1e-8) + 0.1 * old
            m[at, :] = new_m
            v[at, :] = new_v
            new[at, :] = (old - 0.02 * step).astype(BF16)

        chunks(new.shape[0], body)

    def update(i):
        layer, which = ORDER[i]
        for copy in load(i):
            copy.wait()
        if layer == 1:
            step_block(mine(i), *holds(i), mine(i))
            return

        @pl.when(outer)
        def _():
            step_block(mine(i), *holds(i), mine(i))

        @pl.when(inner)
        def _():
            give(which).wait_recv()
            step_block(rs[which].at[0, 2], *holds(i), mine(i))

    def keep(i, block, src):
        layer, which = ORDER[i]
        return pltpu.make_async_copy(src, w_out[which].at[layer, block, k], keep_sem.at[i, jnp.where(block == own, 0, 1)])

    def mine(i):
        layer, which = ORDER[i]
        return full[which].at[layer, own, k]

    def extra(i):
        _, which = ORDER[i]
        rows = m_in[which].shape[1]
        m, v = (acc.at[1024:1280], acc.at[1280:1536]) if which == 2 else (moments.at[0], moments.at[1])
        new, old = rs[which].at[0, 2], rs[which].at[0, 3]
        first = pl.multiple_of((2 * blk(1) + k) * rows, 16)
        for copy in lend(which):
            copy.wait_recv()
        loads = (
            pltpu.make_async_copy(m_lent[which], m, extra_sem.at[which, 0]),
            pltpu.make_async_copy(v_lent[which], v, extra_sem.at[which, 1]),
            pltpu.make_async_copy(w_in[which].at[0, pl.ds(first, rows)], old, extra_sem.at[which, 2]),
        )
        for copy in loads:
            copy.start()
        for copy in loads:
            copy.wait()
        step_block(full[which].at[0, blk(1), k], m, v, old, new)
        keep(i, blk(1), new).start()
        across_copy(i, blk(1), new).start()

    def pass_on(i, block, which_way, to, plane, src):
        layer, which = ORDER[i]
        here = w_out[which].at[layer, block, plane]
        return remote(here if src is None else src, here, g_send.at[i, block, which_way], g_recv.at[i, block, plane], to)

    def ahead_copy(i, block, src=None):
        return pass_on(i, block, 0, device(ahead, k), k, src)

    def back_copy(i, block, src=None):
        return pass_on(i, block, 1, device(back, k), k, src)

    def across_copy(i, block, src=None):
        return pass_on(i, block, 2, device(z, 1 - k), k, src)

    for s in range(N + 3):
        if s < N:
            before = {2: 1, 4: 2, 5: 4}.get(s)
            if before is not None:
                for copy in store(before):
                    copy.wait()
                for copy in load(s):
                    copy.start()
            update(s)
            if ORDER[s][0] == 1:

                @pl.when(inner)
                def _():
                    back_copy(s, own, mine(s)).start()

            ahead_copy(s, own, mine(s)).start()
            across_copy(s, own, mine(s)).start()
            if s in (1, 2, 3):

                @pl.when(outer)
                def _():
                    give((2, 0, 1)[s - 1]).start()

            keep(s, own, mine(s)).start()
            for copy in store(s):
                copy.start()
        if 0 <= s - 1 < N:
            i = s - 1
            if ORDER[i][0] == 1:

                @pl.when(outer)
                def _():
                    ahead_copy(i, blk(1)).wait_recv()
                    across_copy(i, blk(1)).start()

            @pl.when(inner)
            def _():
                ahead_copy(i, blk(2)).wait_recv()
                back_copy(i, blk(2)).start()
                across_copy(i, blk(2)).start()
                ahead_copy(i, blk(0)).wait_recv()
                ahead_copy(i, blk(0)).start()
                across_copy(i, blk(0)).start()

        if s >= N:
            i = (3, 4, 5)[s - N]
            if i == 4:
                for copy in store(5):
                    copy.wait()

            @pl.when(outer)
            def _():
                extra(i)

        if 0 <= s - 2 < N:
            i = s - 2

            @pl.when(outer)
            def _():
                ahead_copy(i, blk(2)).wait_recv()
                across_copy(i, blk(2)).start()

            @pl.when(inner)
            def _():
                ahead_copy(i, blk(3)).wait_recv()
                back_copy(i, blk(3)).start()
                across_copy(i, blk(3)).start()

        if 0 <= s - 3 < N:
            i = s - 3

            @pl.when(outer)
            def _():
                ahead_copy(i, blk(3)).wait_recv()
                across_copy(i, blk(3)).start()

    for p in range(1, 8):
        norm(p, me).wait_send()
    for i in range(N):
        layer, which = ORDER[i]
        if i in (0, 3):
            for copy in store(i):
                copy.wait()
        keep(i, own, mine(i)).wait()
        for b in range(4):
            pass_on(i, b, 2, device(z, 1 - k), 1 - k, None).wait_recv()
            across_copy(i, b).wait_send()
        ahead_copy(i, own).wait_send()
        if layer == 0:

            @pl.when(outer)
            def _():
                keep(i, blk(1), rs[which].at[0, 2]).wait()
                give(which).wait_send()

        @pl.when(inner)
        def _():
            ahead_copy(i, blk(0)).wait_send()
            for b in range(1 if layer == 1 else 2, 4):
                back_copy(i, blk(b)).wait_send()
            if layer == 0:
                for copy in lend(which):
                    copy.wait_send()


def copy_kernel(*refs):
    ins, outs, held, (in_sem, out_sem) = refs[:9], refs[9:18], refs[18:27], refs[27:]

    def each(sem, sources, targets):
        return [
            pltpu.make_async_copy(sources[n].at[layer], targets[n].at[layer], sem.at[n, layer])
            for n in range(9)
            for layer in range(2)
        ]

    loads, stores = each(in_sem, ins, held), each(out_sem, held, outs)
    for load in loads:
        load.start()
    for load, store in zip(loads, stores):
        load.wait()
        store.start()
    for store in stores:
        store.wait()


def copied(arrays):
    any_space = pl.BlockSpec(memory_space=pl.ANY)
    return pl.pallas_call(
        copy_kernel,
        out_shape=[jax.ShapeDtypeStruct(t.shape, t.dtype) for t in arrays],
        in_specs=[any_space] * 9,
        out_specs=[any_space] * 9,
        scratch_shapes=[pltpu.VMEM(t.shape, t.dtype) for t in arrays] + [pltpu.SemaphoreType.DMA((9, 2))] * 2,
        compiler_params=pltpu.CompilerParams(vmem_limit_bytes=67043328),
        name="results",
    )(*arrays)


def solution(mesh):
    def step(x, dy, *arrays):
        weights = arrays[:3]
        dims = [(w.shape[0], w.shape[1] // 8, w.shape[2]) for w in weights]
        count = float(sum(w.size for w in weights))
        any_space = pl.BlockSpec(memory_space=pl.ANY)
        dma = pltpu.SemaphoreType.DMA
        out = pl.pallas_call(
            functools.partial(step_kernel, count),
            out_shape=[jax.ShapeDtypeStruct((l, 4, 2, r, c), BF16) for l, r, c in dims]
            + [jax.ShapeDtypeStruct(d, F32) for d in dims] * 2
            + [jax.ShapeDtypeStruct(d[1:], F32) for d in dims] * 2,
            in_specs=[any_space] * 11,
            out_specs=[any_space] * 15,
            scratch_shapes=[pltpu.VMEM((l, 4, 2, r, c), BF16) for l, r, c in dims]
            + COMPUTE_SCRATCH
            + [pltpu.VMEM((l, 4, r, c), BF16) for l, r, c in dims]
            + [pltpu.VMEM((l, 5, r, c), BF16) for l, r, c in dims]
            + [
                pltpu.VMEM((2, D // 8, FF), F32),
                pltpu.VMEM((8, 128), F32),
                pltpu.VMEM((8, 8, 128), F32),
                dma((N, 3)),
                dma((N, 2)),
                dma((UNITS, 3)),
                dma((UNITS, 3)),
                dma((UNITS, PIECES, 3)),
                dma((UNITS, PIECES, 5)),
                dma((7,)),
                dma((8,)),
                dma((N, 4, 3)),
                dma((N, 4, 2)),
                dma((3, 2)),
                dma((3, 2)),
                dma((PARTS, PIECES)),
                dma((PARTS, PIECES)),
                dma((N, 2)),
                dma((3, 3)),
                dma((3,)),
                dma((3,)),
            ],
            compiler_params=pltpu.CompilerParams(collective_id=0, has_side_effects=True, vmem_limit_bytes=67043328),
            name="training_step",
        )(x[0], dy[0], *arrays)
        return tuple(copied([o.reshape(w.shape) for o, w in zip(out[:3], weights)] + list(out[3:9])))

    every, rows, whole = P(("rep", "dp")), P(None, "dp"), P(None)
    return jax.shard_map(
        step,
        mesh=mesh,
        in_specs=(every, every, whole, whole, whole) + (rows,) * 6,
        out_specs=(P("rep"),) * 3 + (P("rep", "dp"),) * 6,
        check_vma=False,
    )
```

```python
import functools

import jax
import jax.numpy as jnp
from jax import lax
from jax.experimental import pallas as pl
from jax.experimental.pallas import tpu as pltpu
from jax.sharding import PartitionSpec as P

NAMES = ("w_gate", "w_up", "w_down")
MESH = pl.DeviceIdType.MESH
F32, BF16 = jnp.float32, jnp.bfloat16
ORDER = ((1, 2), (1, 0), (1, 1), (0, 2), (0, 0), (0, 1))
N = len(ORDER)


def chunks(rows, body):
    @pl.loop(0, rows // 16)
    def _(t):
        body(pl.ds(pl.multiple_of(t * 16, 16), 16))


TOKENS, D, FF = 2048, 640, 2048
T, CH = 512, 512
PARTS = FF // CH
STATIC_UNROLL = 1


def nt(a, b):
    return lax.dot_general(a, b, (((1,), (1,)), ((), ())), preferred_element_type=F32)


def nn(a, b):
    return jnp.dot(a, b, preferred_element_type=F32)


def tile(t, size=T):
    return pl.ds(pl.multiple_of(t * size, size), size)


def scale_of(wide):
    return lax.rsqrt(jnp.mean(wide * wide, -1, keepdims=True) + 1e-6)


def compute(x_hbm, dy_hbm, w_hbm, full, h, a, a_t, d, d_t, acc, hid, dgate, dup, wg, wu, wd, in_sem, w_sem, after_tile, after_part):
    def weights(number):
        layer = jnp.where(number // PARTS == 1, 1, 0)
        at, slot = tile(lax.rem(number, PARTS), CH), lax.rem(number, 2)
        return (
            pltpu.make_async_copy(w_hbm[0].at[layer, :, at], wg.at[slot], w_sem.at[slot, 0]),
            pltpu.make_async_copy(w_hbm[1].at[layer, :, at], wu.at[slot], w_sem.at[slot, 1]),
            pltpu.make_async_copy(w_hbm[2].at[layer, at, :], wd.at[slot], w_sem.at[slot, 2]),
        )

    def next_weights(number):
        for copy in weights(number):
            copy.wait()

        @pl.when(number + 1 < 3 * PARTS)
        def _():
            for copy in weights(number + 1):
                copy.start()

        return lax.rem(number, 2)

    def norm_tile(at, wide):
        value = (wide * scale_of(wide)).astype(BF16)
        a[at, :] = value
        a_t[:, at] = value.T

    def load_tile(t):
        return pltpu.make_async_copy(x_hbm.at[tile(t)], h.at[tile(t)], in_sem.at[2 + t])

    load_x = pltpu.make_async_copy(x_hbm, h, in_sem.at[0])
    load_dy = pltpu.make_async_copy(dy_hbm, d, in_sem.at[1])
    load_x.start()
    load_dy.start()
    for copy in weights(0):
        copy.start()
    load_x.wait()

    @pl.loop(0, TOKENS // T)
    def _(t):
        wide = h[tile(t), :].astype(F32)
        a[tile(t), :] = (wide * scale_of(wide)).astype(BF16)

    @pl.loop(0, PARTS)
    def _(c):
        slot = next_weights(c)

        def forward(t, first):
            at = tile(t)
            gate, up = nn(a[at, :], wg[slot]), nn(a[at, :], wu[slot])
            value = nn((gate * jax.nn.sigmoid(gate) * up).astype(BF16), wd[slot])
            if first:
                acc[at, :] = value
            else:
                acc[at, :] += value

        @pl.when(c == 0)
        def _():
            @pl.loop(0, TOKENS // T, unroll=STATIC_UNROLL)
            def _(t):
                forward(t, True)

        @pl.when(c > 0)
        def _():
            @pl.loop(0, TOKENS // T, unroll=STATIC_UNROLL)
            def _(t):
                forward(t, False)

    load_dy.wait()

    @pl.loop(0, TOKENS // T)
    def _(t):
        at = tile(t)
        value = h[at, :].astype(F32) + acc[at, :].astype(BF16).astype(F32)
        value = value.astype(BF16)
        h[at, :] = value
        norm_tile(at, value.astype(F32))
        d_t[:, at] = d[at, :].T
        acc[at, :] = jnp.zeros((T, D), F32)

    def backward(layer):
        @pl.loop(0, PARTS)
        def _(c):
            number = (2 - layer) * PARTS + c
            slot = next_weights(number)

            @pl.loop(0, TOKENS // T // STATIC_UNROLL)
            def _(pair):
                for half in range(STATIC_UNROLL):
                    at = tile(pair * STATIC_UNROLL + half)
                    gate, up = nn(a[at, :], wg[slot]), nn(a[at, :], wu[slot])
                    back = nt(d[at, :], wd[slot]).astype(BF16).astype(F32)
                    sig = jax.nn.sigmoid(gate)
                    silu = gate * sig
                    hid[at, :] = (silu * up).astype(BF16)
                    by_up = (back * silu).astype(BF16)
                    by_gate = (back * up * (sig + silu * (1.0 - sig))).astype(BF16)
                    dup[at, :] = by_up
                    dgate[at, :] = by_gate
                    if layer == 1:
                        acc[at, :] += nt(by_gate, wg[slot]) + nt(by_up, wu[slot])
                after_tile(number - PARTS, pair)

            @pl.loop(0, CH // 256)
            def _(n):
                here = tile(n, 256)
                there = pl.ds(pl.multiple_of(c * CH + n * 256, 256), 256)
                full[2][layer, c, n] = nn(d_t[...], hid[:, here]).astype(BF16).T
                full[0][layer, :, :, :, there] = nn(a_t[...], dgate[:, here]).astype(BF16).reshape(4, 2, D // 8, 256)
                full[1][layer, :, :, :, there] = nn(a_t[...], dup[:, here]).astype(BF16).reshape(4, 2, D // 8, 256)

            after_part(number - PARTS)

    backward(1)

    @pl.loop(0, TOKENS // T)
    def _(t):
        at = tile(t)
        wide = h[at, :].astype(F32)
        scale = scale_of(wide)
        by_a = acc[at, :].astype(BF16).astype(F32)
        by_h = scale * by_a - wide * (scale * scale * scale * jnp.mean(by_a * wide, -1, keepdims=True))
        value = (d[at, :].astype(F32) + by_h.astype(BF16).astype(F32)).astype(BF16)
        d[at, :] = value
        d_t[:, at] = value.T
        load_tile(t).start()

    @pl.loop(0, TOKENS // T)
    def _(t):
        load_tile(t).wait()
        norm_tile(tile(t), h[tile(t), :].astype(F32))

    backward(0)


COMPUTE_SCRATCH = [
    pltpu.VMEM((TOKENS, D), BF16),
    pltpu.VMEM((TOKENS, D), BF16),
    pltpu.VMEM((D, TOKENS), BF16),
    pltpu.VMEM((TOKENS, D), BF16),
    pltpu.VMEM((D, TOKENS), BF16),
    pltpu.VMEM((TOKENS, D), F32),
    pltpu.VMEM((TOKENS, CH), BF16),
    pltpu.VMEM((TOKENS, CH), BF16),
    pltpu.VMEM((TOKENS, CH), BF16),
    pltpu.VMEM((2, D, CH), BF16),
    pltpu.VMEM((2, D, CH), BF16),
    pltpu.VMEM((2, CH, D), BF16),
    pltpu.SemaphoreType.DMA((2 + TOKENS // T,)),
    pltpu.SemaphoreType.DMA((2, 3)),
]


LAG = 2
UNITS = 2 * PARTS
QUARTERS, ROWS = 4, FF // 32
PIECES = 2 + QUARTERS


def step_kernel(count, x_hbm, dy_hbm, *refs):
    w_in, m_in, v_in, refs = refs[:3], refs[3:6], refs[6:9], refs[9:]
    w_out, m_out, v_out, m_lent, v_lent, refs = refs[:3], refs[3:6], refs[6:9], refs[9:12], refs[12:15], refs[15:]
    full, refs = refs[:3], refs[3:]
    scratch, refs = refs[: len(COMPUTE_SCRATCH)], refs[len(COMPUTE_SCRATCH) :]
    xs, rs, refs = refs[:3], refs[3:6], refs[6:]
    moments, squares, norms, load_sem, store_sem, x_send, x_recv, r_send, r_recv, n_send, n_recv, g_send, g_recv, refs = *refs[:13], refs[13:]
    lend_send, lend_recv, sum_send, sum_recv, keep_sem, extra_sem, give_send, give_recv = refs
    a, a_t, acc = scratch[1], scratch[2], scratch[5]

    rep, me = lax.axis_index("rep"), lax.axis_index("dp")
    z, k = me // 2, lax.rem(me, 2)
    flip = z >= 2
    inner = jnp.logical_or(z == 1, z == 2)
    outer = jnp.logical_not(inner)

    def blk(mirrored):
        return jnp.where(flip, 3 - mirrored, mirrored)

    own = jnp.where(inner, blk(1), blk(0))
    ahead = jnp.where(flip, z - 1, z + 1)
    back = jnp.where(outer, z, jnp.where(flip, z + 1, z - 1))

    def device(zz, kk):
        return (rep, 2 * zz + kk)

    def remote(src, dst, send, recv, to):
        return pltpu.make_async_remote_copy(
            src_ref=src, dst_ref=dst, send_sem=send, recv_sem=recv, device_id=to, device_id_type=MESH
        )


    def place(u):
        c = lax.rem(u, PARTS)
        return 1 - u // PARTS, c, tile(c, CH)

    def exchange(u):
        layer, c, at = place(u)
        to = device(z, 1 - k)
        return [
            remote(full[m].at[layer, :, 1 - k, :, at], xs[m].at[layer, :, :, at], x_send.at[u, m], x_recv.at[u, m], to)
            for m in range(2)
        ] + [remote(full[2].at[layer, c, 1 - k], xs[2].at[layer, c], x_send.at[u, 2], x_recv.at[u, 2], to)]

    def hop(u, m, block, slot, send, to):
        layer, c, at = place(u)
        sems = r_send.at[u, m, send], r_recv.at[u, m, slot], device(to, k)
        if m >= 2:
            rows = pl.ds((m - 2) * ROWS, ROWS)
            return remote(full[2].at[layer, c, k, rows], rs[2].at[layer, slot, rows], *sems)
        return remote(full[m].at[layer, block, k, :, at], rs[m].at[layer, slot, :, at], *sems)

    def each(u, block, body):
        body(0)
        body(1)

        @pl.when(lax.rem(u, PARTS) == block)
        def _():
            for m in range(2, PIECES):
                body(m)

    def add(u, m, block, slots, square=False):
        layer, c, at = place(u)
        w = min(m, 2)

        def part(rows, columns):
            x = xs[w][layer, block, rows, columns]
            total = full[w][layer, block, k, rows, columns].astype(F32) + x.astype(F32)
            for slot in slots:
                total += rs[w][layer, slot, rows, columns].astype(F32)
            total = total.astype(BF16)
            full[w][layer, block, k, rows, columns] = total
            if square:
                total = total.astype(F32)
                total = total * total
                folded = total[:8]
                for r in range(1, total.shape[0] // 8):
                    folded += total[r * 8 : (r + 1) * 8]
                sums = squares[...]
                for q in range(total.shape[1] // 128):
                    sums += folded[:, q * 128 : (q + 1) * 128]
                squares[...] = sums

        if m < 2:
            part(pl.ds(0, D // 8), at)
        else:
            part(pl.ds((m - 2) * ROWS, ROWS), pl.ds(0, D))


    def when(condition, body):
        if not isinstance(condition, bool):
            pl.when(condition)(body)
        elif condition:
            body()

    def lend(which):
        to = device(back, k)
        return (
            remote(m_in[which].at[0], m_lent[which], lend_send.at[which, 0], lend_recv.at[which, 0], to),
            remote(v_in[which].at[0], v_lent[which], lend_send.at[which, 1], lend_recv.at[which, 1], to),
        )

    def partial(u, m):
        _, c, at = place(u)
        sems = sum_send.at[c, m], sum_recv.at[c, m], device(back, k)
        if m >= 2:
            rows = pl.ds((m - 2) * ROWS, ROWS)
            return remote(full[2].at[0, c, k, rows], rs[2].at[0, 1, rows], *sems)
        return remote(full[m].at[0, own, k, :, at], rs[m].at[0, 1, :, at], *sems)

    def give(which):
        here = full[which].at[0, blk(1), k]
        return remote(here, rs[which].at[0, 2], give_send.at[which], give_recv.at[which], device(ahead, k))

    def send_out(u):
        for copy in exchange(u):
            copy.wait_recv()

        @pl.when(outer)
        def _():
            for j in range(3):

                def body(m):
                    add(u, m, blk(3 - j), ())
                    hop(u, m, blk(3 - j), j, j, ahead).start()

                when(j < 2 or u < PARTS, lambda: each(u, blk(3 - j), body))

    def pass_sum(u, j):
        block, come, go, to = ((3, 0, 3, ahead), (2, 1, 4, ahead), (0, 3, 0, back))[j]

        @pl.when(inner)
        def _():
            def body(m):
                hop(u, m, blk(block), come, j, ahead).wait_recv()
                add(u, m, blk(block), (come,))
                hop(u, m, blk(block), go, j, to).start()

            each(u, blk(block), body)

    def finish(u):
        @pl.when(outer)
        def _():
            def body(m):
                hop(u, m, own, 0, 0, ahead).wait_recv()
                add(u, m, own, (0,), True)

            each(u, own, body)

            def theirs(m):
                partial(u, m).wait_recv()
                add(u, m, blk(1), (1,), True)

            when(u >= PARTS, lambda: each(u, blk(1), theirs))

        def body(m):
            hop(u, m, own, 2, 2, ahead).wait_recv()
            hop(u, m, own, 4, 2, ahead).wait_recv()
            add(u, m, own, (2, 4), True)

        when(u < PARTS, lambda: pl.when(inner)(lambda: each(u, own, body)))

    def pass_out(u):
        @pl.when(inner)
        def _():
            def body(m):
                hop(u, m, own, 4, 2, ahead).wait_recv()
                add(u, m, own, (4,))
                partial(u, m).start()

            each(u, own, body)

    def sent(u):
        for copy in exchange(u):
            copy.wait_send()

        @pl.when(outer)
        def _():
            for j in range(3):
                when(
                    j < 2 or u < PARTS,
                    lambda: each(u, blk(3 - j), lambda m: hop(u, m, blk(3 - j), j, j, ahead).wait_send()),
                )

        @pl.when(inner)
        def _():
            for j, block in enumerate((3, 2, 0)):
                each(u, blk(block), lambda m: hop(u, m, blk(block), 0, j, ahead).wait_send())
            when(u >= PARTS, lambda: each(u, own, lambda m: partial(u, m).wait_send()))

    def after_part(u):
        for copy in exchange(u):
            copy.start()

    def beside(u, p):
        @pl.when(jnp.logical_and(p == 0, u >= 1))
        def _():
            send_out(u - 1)

        @pl.when(jnp.logical_and(p == 1, u >= LAG))
        def _():
            pass_sum(u - LAG, 0)

        @pl.when(jnp.logical_and(p == 2, u >= LAG))
        def _():
            pass_sum(u - LAG, 1)

        @pl.when(jnp.logical_and(p == 2, u >= LAG + 2))
        def _():
            finish(u - LAG - 2)

        @pl.when(jnp.logical_and(p == 3, u >= LAG + 1))
        def _():
            pass_sum(u - LAG - 1, 2)

        @pl.when(jnp.logical_and(p == 3, u >= LAG + PARTS + 1))
        def _():
            pass_out(u - LAG - 1)

    squares[...] = jnp.zeros_like(squares)
    barrier = pltpu.get_barrier_semaphore()
    for p in range(1, 8):
        pl.semaphore_signal(barrier, inc=1, device_id=(rep, lax.rem(me + p, 8)), device_id_type=MESH)
    pl.semaphore_wait(barrier, 7)

    @pl.when(inner)
    def _():
        for which in range(3):
            for copy in lend(which):
                copy.start()

    compute(x_hbm, dy_hbm, w_in, full, *scratch, beside, after_part)


    def holds(i):
        layer, which = ORDER[i]
        if which == 2:
            first = 512 * layer
            return acc.at[first : first + 256], acc.at[first + 256 : first + 512], a.at[256 * layer : 256 * layer + 256]
        old = (2 * layer + which) * (D // 8)
        return moments.at[0], moments.at[1], a_t.at[old : old + D // 8]

    def load(i):
        layer, which = ORDER[i]
        rows = m_in[which].shape[1]
        m, v, old = holds(i)
        return (
            pltpu.make_async_copy(m_in[which].at[layer], m, load_sem.at[i, 0]),
            pltpu.make_async_copy(v_in[which].at[layer], v, load_sem.at[i, 1]),
            pltpu.make_async_copy(w_in[which].at[layer, pl.ds(pl.multiple_of(me * rows, 16), rows)], old, load_sem.at[i, 2]),
        )

    def store(i):
        layer, which = ORDER[i]
        m, v, _ = holds(i)
        return (
            pltpu.make_async_copy(m, m_out[which].at[layer], store_sem.at[i, 0]),
            pltpu.make_async_copy(v, v_out[which].at[layer], store_sem.at[i, 1]),
        )

    for i in (0, 1, 3):
        for copy in load(i):
            copy.start()

    send_out(UNITS - 1)
    pass_sum(6, 0)
    pass_sum(5, 2)
    pass_out(5)
    pass_sum(6, 1)
    pass_sum(7, 0)
    pass_sum(6, 2)
    pass_out(6)
    finish(4)
    pass_sum(7, 1)
    finish(5)
    pass_sum(7, 2)
    pass_out(7)
    finish(6)
    finish(7)

    norms[me] = squares[...]

    def norm(p, src):
        return remote(norms.at[src], norms.at[src], n_send.at[p - 1], n_recv.at[src], (rep, lax.rem(me + p, 8)))

    for p in range(1, 8):
        norm(p, me).start()
    for p in range(1, 8):
        norm(p, lax.rem(me + p, 8)).wait_recv()
    total = norms[0]
    for other in range(1, 8):
        total += norms[other]
    ss = jnp.sum(total, keepdims=True)
    factor = jnp.minimum(1.0, 0.5 * lax.rsqrt(ss / count + 1e-30))

    def step_block(grad, m, v, w, new):
        def body(at):
            g = grad[at, :].astype(F32) * factor
            new_m = 0.9 * m[at, :] + 0.1 * g
            new_v = 0.95 * v[at, :] + 0.05 * g * g
            old = w[at, :].astype(F32)
            step = new_m * lax.rsqrt(new_v + 1e-8) + 0.1 * old
            m[at, :] = new_m
            v[at, :] = new_v
            new[at, :] = (old - 0.02 * step).astype(BF16)

        chunks(new.shape[0], body)

    def update(i):
        layer, which = ORDER[i]
        for copy in load(i):
            copy.wait()
        if layer == 1:
            step_block(mine(i), *holds(i), mine(i))
            return

        @pl.when(outer)
        def _():
            step_block(mine(i), *holds(i), mine(i))

        @pl.when(inner)
        def _():
            give(which).wait_recv()
            step_block(rs[which].at[0, 2], *holds(i), mine(i))

    def keep(i, block, src):
        layer, which = ORDER[i]
        return pltpu.make_async_copy(src, w_out[which].at[layer, block, k], keep_sem.at[i, jnp.where(block == own, 0, 1)])

    def mine(i):
        layer, which = ORDER[i]
        return full[which].at[layer, own, k]

    def extra(i):
        _, which = ORDER[i]
        rows = m_in[which].shape[1]
        m, v = (acc.at[1024:1280], acc.at[1280:1536]) if which == 2 else (moments.at[0], moments.at[1])
        new, old = rs[which].at[0, 2], rs[which].at[0, 3]
        first = pl.multiple_of((2 * blk(1) + k) * rows, 16)
        for copy in lend(which):
            copy.wait_recv()
        loads = (
            pltpu.make_async_copy(m_lent[which], m, extra_sem.at[which, 0]),
            pltpu.make_async_copy(v_lent[which], v, extra_sem.at[which, 1]),
            pltpu.make_async_copy(w_in[which].at[0, pl.ds(first, rows)], old, extra_sem.at[which, 2]),
        )
        for copy in loads:
            copy.start()
        for copy in loads:
            copy.wait()
        step_block(full[which].at[0, blk(1), k], m, v, old, new)
        keep(i, blk(1), new).start()
        across_copy(i, blk(1), new).start()

    def pass_on(i, block, which_way, to, plane, src):
        layer, which = ORDER[i]
        here = w_out[which].at[layer, block, plane]
        return remote(here if src is None else src, here, g_send.at[i, block, which_way], g_recv.at[i, block, plane], to)

    def ahead_copy(i, block, src=None):
        return pass_on(i, block, 0, device(ahead, k), k, src)

    def back_copy(i, block, src=None):
        return pass_on(i, block, 1, device(back, k), k, src)

    def across_copy(i, block, src=None):
        return pass_on(i, block, 2, device(z, 1 - k), k, src)

    for s in range(N + 3):
        if s == 3:

            @pl.loop(0, UNITS)
            def _(u):
                sent(u)

        if s < N:
            before = {2: 1, 4: 2, 5: 4}.get(s)
            if before is not None:
                for copy in store(before):
                    copy.wait()
                for copy in load(s):
                    copy.start()
            update(s)
            if ORDER[s][0] == 1:

                @pl.when(inner)
                def _():
                    back_copy(s, own, mine(s)).start()

            ahead_copy(s, own, mine(s)).start()
            across_copy(s, own, mine(s)).start()
            if s in (1, 2, 3):

                @pl.when(outer)
                def _():
                    give((2, 0, 1)[s - 1]).start()

            keep(s, own, mine(s)).start()
            for copy in store(s):
                copy.start()
        if 0 <= s - 1 < N:
            i = s - 1
            if ORDER[i][0] == 1:

                @pl.when(outer)
                def _():
                    ahead_copy(i, blk(1)).wait_recv()
                    across_copy(i, blk(1)).start()

            @pl.when(inner)
            def _():
                ahead_copy(i, blk(2)).wait_recv()
                back_copy(i, blk(2)).start()
                across_copy(i, blk(2)).start()
                ahead_copy(i, blk(0)).wait_recv()
                ahead_copy(i, blk(0)).start()
                across_copy(i, blk(0)).start()

        if s >= N:
            i = (3, 4, 5)[s - N]
            if i == 4:
                for copy in store(5):
                    copy.wait()

            @pl.when(outer)
            def _():
                extra(i)

        if 0 <= s - 2 < N:
            i = s - 2

            @pl.when(outer)
            def _():
                ahead_copy(i, blk(2)).wait_recv()
                across_copy(i, blk(2)).start()

            @pl.when(inner)
            def _():
                ahead_copy(i, blk(3)).wait_recv()
                back_copy(i, blk(3)).start()
                across_copy(i, blk(3)).start()

        if 0 <= s - 3 < N:
            i = s - 3

            @pl.when(outer)
            def _():
                ahead_copy(i, blk(3)).wait_recv()
                across_copy(i, blk(3)).start()

    for p in range(1, 8):
        norm(p, me).wait_send()
    for i in range(N):
        layer, which = ORDER[i]
        if i in (0, 3):
            for copy in store(i):
                copy.wait()
        keep(i, own, mine(i)).wait()
        for b in range(4):
            pass_on(i, b, 2, device(z, 1 - k), 1 - k, None).wait_recv()
            across_copy(i, b).wait_send()
        ahead_copy(i, own).wait_send()
        if layer == 0:

            @pl.when(outer)
            def _():
                keep(i, blk(1), rs[which].at[0, 2]).wait()
                give(which).wait_send()

        @pl.when(inner)
        def _():
            ahead_copy(i, blk(0)).wait_send()
            for b in range(1 if layer == 1 else 2, 4):
                back_copy(i, blk(b)).wait_send()
            if layer == 0:
                for copy in lend(which):
                    copy.wait_send()


def copy_kernel(*refs):
    ins, outs, held, (in_sem, out_sem) = refs[:9], refs[9:18], refs[18:27], refs[27:]

    def each(sem, sources, targets):
        return [
            pltpu.make_async_copy(sources[n].at[layer], targets[n].at[layer], sem.at[n, layer])
            for n in (3, 4, 5, 0, 1, 2, 6, 7, 8)
            for layer in range(2)
        ]

    loads, stores = each(in_sem, ins, held), each(out_sem, held, outs)
    for load in loads:
        load.start()
    for load, store in zip(loads, stores):
        load.wait()
        store.start()
    for store in stores:
        store.wait()


def copied(arrays):
    any_space = pl.BlockSpec(memory_space=pl.ANY)
    return pl.pallas_call(
        copy_kernel,
        out_shape=[jax.ShapeDtypeStruct(t.shape, t.dtype) for t in arrays],
        in_specs=[any_space] * 9,
        out_specs=[any_space] * 9,
        scratch_shapes=[pltpu.VMEM(t.shape, t.dtype) for t in arrays] + [pltpu.SemaphoreType.DMA((9, 2))] * 2,
        compiler_params=pltpu.CompilerParams(vmem_limit_bytes=67043328),
        name="results",
    )(*arrays)


def solution(mesh):
    def step(x, dy, *arrays):
        weights = arrays[:3]
        dims = [(w.shape[0], w.shape[1] // 8, w.shape[2]) for w in weights]
        count = float(sum(w.size for w in weights))
        any_space = pl.BlockSpec(memory_space=pl.ANY)
        dma = pltpu.SemaphoreType.DMA
        out = pl.pallas_call(
            functools.partial(step_kernel, count),
            out_shape=[jax.ShapeDtypeStruct((l, 4, 2, r, c), BF16) for l, r, c in dims]
            + [jax.ShapeDtypeStruct(d, F32) for d in dims] * 2
            + [jax.ShapeDtypeStruct(d[1:], F32) for d in dims] * 2,
            in_specs=[any_space] * 11,
            out_specs=[any_space] * 15,
            scratch_shapes=[pltpu.VMEM((l, 4, 2, r, c), BF16) for l, r, c in dims]
            + COMPUTE_SCRATCH
            + [pltpu.VMEM((l, 4, r, c), BF16) for l, r, c in dims]
            + [pltpu.VMEM((l, 5, r, c), BF16) for l, r, c in dims]
            + [
                pltpu.VMEM((2, D // 8, FF), F32),
                pltpu.VMEM((8, 128), F32),
                pltpu.VMEM((8, 8, 128), F32),
                dma((N, 3)),
                dma((N, 2)),
                dma((UNITS, 3)),
                dma((UNITS, 3)),
                dma((UNITS, PIECES, 3)),
                dma((UNITS, PIECES, 5)),
                dma((7,)),
                dma((8,)),
                dma((N, 4, 3)),
                dma((N, 4, 2)),
                dma((3, 2)),
                dma((3, 2)),
                dma((PARTS, PIECES)),
                dma((PARTS, PIECES)),
                dma((N, 2)),
                dma((3, 3)),
                dma((3,)),
                dma((3,)),
            ],
            compiler_params=pltpu.CompilerParams(collective_id=0, has_side_effects=True, vmem_limit_bytes=67043328),
            name="training_step",
        )(x[0], dy[0], *arrays)
        return tuple(copied([o.reshape(w.shape) for o, w in zip(out[:3], weights)] + list(out[3:9])))

    every, rows, whole = P(("rep", "dp")), P(None, "dp"), P(None)
    return jax.shard_map(
        step,
        mesh=mesh,
        in_specs=(every, every, whole, whole, whole) + (rows,) * 6,
        out_specs=(P("rep"),) * 3 + (P("rep", "dp"),) * 6,
        check_vma=False,
    )
```
